32 devices in a mesh: tm: 8 (over z, y), space: 4 (over x, core).
Axes of the slice: x: 2, y: 2, z: 4, core: 2. Of those that a mesh axis runs over, the one named last changes fastest.
Arguments:
- density: bfloat16 [2048, 128, 128], P('tm', 'space'), may hold values from -6 to 6
- active: int32 [2048], P('tm'), may hold values from 1 to 128
- neighbours: int32 [128, 8], P('space'), may hold values from 0 to 127, as said below
- near_blocks: bfloat16 [2, 128, 8, 128, 128], P(None, 'space'), may hold values from -0.125 to 0.125
- to_moments: bfloat16 [64, 128, 128], P(None, 'space'), may hold values from -0.046875 to 0.046875
- from_moments: bfloat16 [64, 128, 128], P(None, 'space'), may hold values from -0.75 to 0.75
- decay_rates: float32 [64], replicated, may hold values from 9.765625e-05 to 0.05, as said below
- lengths: float32 [2048], P('tm'), may hold values from 0.5 to 1024, as said below
Outputs:
- potential: bfloat16 [2048, 128, 128], P('tm', 'space')
The draws below stay inside these ranges and needn't reach their ends.
Inputs may be any that keep to these rules, and one draw needn't show every extreme that they name: `neighbours`: every entry of row c lies within 8 of c; each row names c - 8 and c + 8, clipped to the clusters that exist. `decay_rates`: positive rates. Positive lengths.
All inputs are finite; a program needn't handle non-finite values.
Results may differ from the reference program's by a relative error of at most 0.0085.
Values may be sent and summed in bfloat16 or wider, within the bound.
A program may use at most 128 MiB of HBM per device.

```python
import jax
import jax.numpy as jnp
from jax import lax

ELEM = 128
TERMS = 64
NB = 8
REACH = 8
NT = 2048
NC = 128


def draw_neighbours(key, part):
    offsets = jax.random.randint(key, (NC, NB), -REACH, REACH + 1)
    scores = jax.random.randint(jax.random.fold_in(key, 3), (NC, NB), 0, 1 << 20) * NB + jnp.arange(NB, dtype=jnp.int32)[None, :]
    order = jnp.argsort(scores, axis=1)
    ranks = jnp.argsort(order, axis=1)
    offsets = jnp.where(ranks == 0, REACH, jnp.where(ranks == 1, -REACH, offsets))
    result = jnp.clip(jnp.arange(NC, dtype=jnp.int32)[:, None] + offsets, 0, NC - 1)
    return result.astype(jnp.int32)


def draw_decay_rates(key, part):
    pick = jax.random.uniform(jax.random.fold_in(key, 11), (TERMS,))
    share = 0.5
    slow_log = jax.random.uniform(jax.random.fold_in(key, 12), (TERMS,), minval=jnp.log(0.2 / NT), maxval=jnp.log(0.8 / NT))
    fast_log = jax.random.uniform(jax.random.fold_in(key, 13), (TERMS,), minval=jnp.log(0.02), maxval=jnp.log(0.05))
    return jnp.where(pick < share, jnp.exp(slow_log), jnp.exp(fast_log)).astype(jnp.float32)


def draw_lengths(key, part):
    base = jax.random.uniform(key, (NT,), minval=0.5, maxval=2.0)
    places = jax.random.randint(jax.random.fold_in(key, 5), (3,), 0, NT)
    base = base.at[places].set(jnp.float32(NT // 2))
    return base.astype(jnp.float32)


def touch_ends(values, stream_key, low, high):
    spot = [jax.random.randint(jax.random.fold_in(stream_key, axis), (), 0, length) for axis, length in enumerate(values.shape)]
    longest = values.shape.index(max(values.shape))
    neighbour = spot[:longest] + [(spot[longest] + 1) % values.shape[longest]] + spot[longest + 1:]
    return values.at[tuple(spot)].set(low).at[tuple(neighbour)].set(high)


def levels(stream_key, dims, split, low, largest):
    loudness = 1.0
    for axis_at, parts in split:
        steps = jax.random.uniform(jax.random.fold_in(jax.random.fold_in(stream_key, 6), axis_at), (parts,), jnp.float32, low / len(split), largest / len(split))
        loudness = loudness * jnp.repeat(jnp.exp(steps), dims[axis_at] // parts).reshape((-1,) + (1,) * (len(dims) - 1 - axis_at))
    return loudness


def bell_draw(own_key, dims, deviation, bound, split=(), kind=jnp.bfloat16):
    factor_of = levels(own_key, dims, split, -0.22, 0.18) if split else 1.0
    values = jax.random.normal(own_key, dims, jnp.float32) * deviation * factor_of
    return jnp.minimum(jnp.maximum(values, -bound), bound).astype(kind)


def setup_inputs(seed: int = 0) -> dict:
    key_list = jax.random.split(jax.random.key(seed), 9)
    return {
        "density": bell_draw(key_list[0], (NT, NC, ELEM), 1.0, 6.0, ((0, 8), (1, 4))),
        "active": touch_ends(jax.random.randint(key_list[1], (NT,), 1, NC + 1), jax.random.fold_in(key_list[1], 1), 1, NC).astype(jnp.int32),
        "neighbours": draw_neighbours(jax.random.fold_in(key_list[8], 71), 0),
        "near_blocks": bell_draw(key_list[3], (2, NC, NB, ELEM, ELEM), (2 * NB * ELEM) ** -0.5, 0.125, ((1, 4),)),
        "to_moments": bell_draw(key_list[4], (TERMS, NC, ELEM), (NC * ELEM) ** -0.5, 0.046875, ((1, 4),)),
        "from_moments": bell_draw(key_list[5], (TERMS, NC, ELEM), TERMS ** -0.5, 0.75, ((1, 4),)),
        "decay_rates": draw_decay_rates(jax.random.fold_in(key_list[8], 71), 0),
        "lengths": draw_lengths(jax.random.fold_in(key_list[8], 71), 0),
    }


def reference(density, active, neighbours, near_blocks, to_moments, from_moments, decay_rates, lengths):
    live_mask = (jnp.arange(NC, dtype=jnp.int32)[None, :] < active[:, None]).astype(jnp.bfloat16)
    masked = density * live_mask[:, :, None]
    earlier = jnp.concatenate([jnp.zeros((1, NC, ELEM), jnp.bfloat16), masked[:-1]], 0)

    def one_cluster(cluster):
        chosen = neighbours[cluster]
        current = jnp.take(masked, chosen, axis=1).astype(jnp.float32)
        previous = jnp.take(earlier, chosen, axis=1).astype(jnp.float32)
        blocks = near_blocks[:, cluster].astype(jnp.float32)
        return jnp.einsum('tje,jef->tf', current, blocks[0]) + jnp.einsum('tje,jef->tf', previous, blocks[1])
    near_term = lax.map(one_cluster, jnp.arange(NC, dtype=jnp.int32))
    near_term = jnp.transpose(near_term, (1, 0, 2))
    flat = masked.reshape(NT, NC * ELEM)
    moments = jnp.dot(flat, to_moments.reshape(TERMS, NC * ELEM).T, preferred_element_type=jnp.float32)
    decays = jnp.exp(-decay_rates[None, :] * lengths[:, None])

    def advance(state, inputs):
        factor, moment = inputs
        return (factor * state + moment, state)
    _, far_coeff = lax.scan(advance, jnp.zeros((TERMS,), jnp.float32), (decays, moments))
    scaled = (far_coeff * jnp.sqrt(2.0 * decay_rates)[None, :]).astype(jnp.bfloat16)
    far_term = jnp.dot(scaled, from_moments.reshape(TERMS, NC * ELEM), preferred_element_type=jnp.float32)
    far_term = far_term.reshape(NT, NC, ELEM)
    return (live_mask.astype(jnp.float32)[:, :, None] * (near_term + far_term)).astype(jnp.bfloat16)
```

```python
import functools

import jax
import jax.numpy as jnp
from jax import lax
from jax.experimental import pallas as pl
from jax.experimental.pallas import tpu as pltpu
from jax.sharding import PartitionSpec as P

REACH = 8
PAD = 16
MESH = pl.DeviceIdType.MESH
F32, BF16 = jnp.float32, jnp.bfloat16


def spread(row):
    return jnp.broadcast_to(row, (128, row.shape[1])).T


def kernel(n_tm, n_space, dens, active, nbrs, blocks, to_m, from_m, rates, lengths, out,
           dens_v, flat, work, halo, halo_prev, row_out, row_in, wb, to_raw, from_raw, to_v, from_v,
           near, stage, out_v, act, part_out, part_in, keep, tot_out, tot_in, state,
           in_sem, w_sem, halo_sem, row_sem, part_ssem, part_rsem, tot_ssem, tot_rsem, out_sem):
    T, C, E = dens_v.shape
    M = to_raw.shape[0]
    J = wb.shape[2]
    H = T // 2
    tm, sp = lax.axis_index("tm"), lax.axis_index("space")
    first = sp * C

    c_dens = pltpu.make_async_copy(dens, dens_v, in_sem.at[0])
    c_to = pltpu.make_async_copy(to_m, to_raw, in_sem.at[1])
    c_from = pltpu.make_async_copy(from_m, from_raw, in_sem.at[2])
    c_dens.start()
    c_to.start()
    c_from.start()
    barrier = pltpu.get_barrier_semaphore()

    def greet(t, s):
        pl.semaphore_signal(barrier, inc=1, device_id={"tm": t, "space": s}, device_id_type=MESH)

    for d in range(1, n_space):
        greet(tm, lax.rem(sp + d, n_space))
    for d in range(1, n_tm):
        greet(lax.rem(tm + d, n_tm), sp)
    one, nil = jnp.int32(1), jnp.int32(0)
    has = {-1: (tm > 0, sp > 0), 1: (tm < n_tm - 1, sp < n_space - 1)}
    corners = nil
    for dt in (-1, 1):
        for ds in (-1, 1):
            there = jnp.logical_and(has[dt][0], has[ds][1])
            corners = corners + jnp.where(there, one, nil)

            @pl.when(there)
            def _(dt=dt, ds=ds):
                greet(tm + dt, sp + ds)

    def w_copy(c):
        return pltpu.make_async_copy(blocks.at[:, c], wb.at[:, c], w_sem.at[c])

    for lo, hi in ((REACH, C - REACH), (0, REACH), (C - REACH, C)):
        @pl.loop(lo, hi)
        def _(c):
            w_copy(c).start()

    for h in range(2):
        act[h * H:(h + 1) * H, :] = spread(active[h:h + 1, :].astype(F32))

    c_dens.wait()
    gid = lax.broadcasted_iota(jnp.int32, (C, E), 0).astype(F32) + first.astype(F32)
    row_out[...] = jnp.where(gid < act[T - 1:T, :], dens_v[T - 1].astype(F32), 0.0)
    pl.semaphore_wait(barrier, n_space - 1 + n_tm - 1 + corners)

    def row_copy(ds):
        if ds == 0:
            src, dst = row_out, row_in.at[pl.ds(REACH, C)]
        elif ds == 1:
            src, dst = row_out.at[pl.ds(C - REACH, REACH)], row_in.at[pl.ds(0, REACH)]
        else:
            src, dst = row_out.at[pl.ds(0, REACH)], row_in.at[pl.ds(REACH + C, REACH)]
        return pltpu.make_async_remote_copy(
            src_ref=src, dst_ref=dst, send_sem=row_sem.at[0, ds + 1], recv_sem=row_sem.at[1, ds + 1],
            device_id={"tm": tm + 1, "space": sp + ds}, device_id_type=MESH)

    def halo_copy(ds):
        k = (1 - ds) // 2
        src = dens_v.at[:, pl.ds(C - REACH if ds == 1 else 0, REACH), :]
        return pltpu.make_async_remote_copy(
            src_ref=src, dst_ref=halo.at[k], send_sem=halo_sem.at[0, k], recv_sem=halo_sem.at[1, k],
            device_id={"tm": tm, "space": sp + ds}, device_id_type=MESH)

    def on_space(ds):
        return True if ds == 0 else has[ds][1]

    for ds in (0, 1, -1):
        @pl.when(jnp.logical_and(has[1][0], on_space(ds)))
        def _(ds=ds):
            row_copy(ds).start()
    for ds in (1, -1):
        @pl.when(on_space(ds))
        def _(ds=ds):
            halo_copy(ds).start()

    TB = 16
    @pl.loop(0, T // TB)
    def _(i):
        x = dens_v[pl.ds(i * TB, TB)].astype(F32)
        flat[pl.ds(pl.multiple_of(i * TB * C, TB * C), TB * C), :] = x.reshape(TB * C, E)

    @pl.loop(0, C)
    def _(g):
        x = flat[pl.ds(g, T, stride=C), :]
        live = (first + g).astype(F32) < act[...]
        work[REACH + g, 0:T, :] = jnp.where(live, x, 0.0).astype(BF16)

    def expand(raw, dst):
        @pl.loop(0, M // TB)
        def _(i):
            x = raw[pl.ds(i * TB, TB)].astype(F32)
            flat[pl.ds(pl.multiple_of(i * TB * C, TB * C), TB * C), :] = x.reshape(TB * C, E)

        @pl.loop(0, C)
        def _(g):
            x = flat[pl.ds(g, M, stride=C), :].astype(BF16)
            dst[g, 0:M, :] = x
            dst[g, M:2 * M, :] = x

    c_to.wait()
    expand(to_raw, to_v)

    lane = lax.broadcasted_iota(jnp.int32, (H, 2 * M), 1)
    low = lane < M
    total = jnp.zeros((T, 2 * M), F32)
    GB = 8
    for k in range(C // GB):
        a = jnp.concatenate([work[REACH + k * GB + i, 0:T, :] for i in range(GB)], axis=1)
        b = jnp.concatenate([to_v[k * GB + i] for i in range(GB)], axis=1)
        total = total + lax.dot_general(a, b, (((1,), (1,)), ((), ())), preferred_element_type=F32)
    part = jnp.where(low, total[0:H], total[H:T])
    keep[0] = part
    part_out[...] = part.astype(BF16)

    def part_copy(d):
        return pltpu.make_async_remote_copy(
            src_ref=part_out, dst_ref=part_in.at[sp], send_sem=part_ssem.at[d], recv_sem=part_rsem.at[sp],
            device_id={"tm": tm, "space": lax.rem(sp + d, n_space)}, device_id_type=MESH)

    for d in range(1, n_space):
        part_copy(d).start()

    c_from.wait()
    expand(from_raw, from_v)

    @pl.when(tm == 0)
    def _():
        row_in[...] = jnp.zeros_like(row_in)

    for ds in (0, 1, -1):
        there = has[-1][0] if ds == 0 else jnp.logical_and(has[-1][0], has[-ds][1])

        @pl.when(there)
        def _(ds=ds):
            row_copy(ds).wait_recv()
    top = lax.broadcasted_iota(jnp.int32, (PAD, E), 0) == 0

    @pl.loop(0, C + 2 * REACH)
    def _(g):
        r = jnp.broadcast_to(row_in[pl.ds(g, 1), :], (PAD, E))
        work[g, T:T + PAD, :] = jnp.where(top, r, 0.0).astype(BF16)

    first_row = lax.broadcasted_iota(jnp.int32, (T, E), 0) == 0

    def near_field(c):
        w_copy(c).wait()
        rows = [jnp.clip(nbrs[j, c] - first + REACH, 0, C + 2 * REACH - 1) for j in range(J)]
        picked = jnp.concatenate([work[i] for i in rows], axis=1)
        w = jnp.concatenate([wb[0, c].reshape(J * E, E), wb[1, c].reshape(J * E, E)], axis=1)
        both = jnp.dot(picked, w, preferred_element_type=F32)
        late = both[:, E:]
        late = jnp.where(first_row, late[T:T + 1, :], pltpu.roll(late[0:T], 1, 0))
        near[c] = both[0:T, 0:E] + late

    pl.loop(REACH, C - REACH)(near_field)

    moment = keep[0]
    for d in range(1, n_space):
        k = lax.rem(sp + n_space - d, n_space)
        pltpu.make_async_remote_copy(
            src_ref=part_out, dst_ref=part_in.at[k], send_sem=part_ssem.at[d], recv_sem=part_rsem.at[k],
            device_id={"tm": tm, "space": k}, device_id_type=MESH).wait_recv()
        moment = moment + part_in[k].astype(F32)
    r = rates[...]
    rr = jnp.concatenate([r, r], axis=1)
    span = jnp.where(low, spread(lengths[0:1, :]), spread(lengths[1:2, :]))
    fall = jnp.exp(-rr * span)
    pos = lax.broadcasted_iota(jnp.int32, (H, 2 * M), 0)
    d = 1
    while d < H:
        start = pos < d
        moment = fall * jnp.where(start, 0.0, pltpu.roll(moment, d, 0)) + moment
        fall = fall * jnp.where(start, 1.0, pltpu.roll(fall, d, 0))
        d *= 2
    keep[0] = jnp.where(pos < 1, 0.0, pltpu.roll(moment, 1, 0))
    keep[1] = jnp.where(pos < 1, 1.0, pltpu.roll(fall, 1, 0))
    end_b = jnp.broadcast_to(moment[H - 1:H, :], (8, 2 * M))
    end_a = jnp.broadcast_to(fall[H - 1:H, :], (8, 2 * M))
    low8 = low[0:8]
    roll_b, roll_a = pltpu.roll(end_b, M, 1), pltpu.roll(end_a, M, 1)
    tot_out[0:8] = end_a * roll_a
    tot_out[8:16] = jnp.where(low8, roll_a * end_b + roll_b, end_a * roll_b + end_b)

    def tot_copy(d):
        return pltpu.make_async_remote_copy(
            src_ref=tot_out, dst_ref=tot_in.at[tm], send_sem=tot_ssem.at[d], recv_sem=tot_rsem.at[tm],
            device_id={"tm": tm + d, "space": sp}, device_id_type=MESH)

    for d in range(1, n_tm):
        @pl.when(tm + d < n_tm)
        def _(d=d):
            tot_copy(d).start()

    for ds in (1, -1):
        k = (1 - ds) // 2

        @pl.when(on_space(-ds))
        def _(ds=ds, k=k):
            halo_copy(ds).wait_recv()

            @pl.loop(0, T // 32)
            def _(i):
                x = halo[k, pl.ds(i * 32, 32)].astype(F32)
                flat[pl.ds(pl.multiple_of(i * 32 * REACH, 32 * REACH), 32 * REACH), :] = x.reshape(32 * REACH, E)

            begin = 0 if k == 0 else REACH + C

            @pl.loop(0, REACH)
            def _(g):
                x = flat[pl.ds(g, T, stride=REACH), :]
                live = (first - REACH + begin + g).astype(F32) < act[...]
                work[begin + g, 0:T, :] = jnp.where(live, x, 0.0).astype(BF16)

    @pl.loop(0, 2 * REACH)
    def _(i):
        near_field(jnp.where(i < REACH, i, i + C - 2 * REACH))

    state[...] = jnp.zeros_like(state)
    for k in range(n_tm - 1):
        @pl.when(k < tm)
        def _(k=k):
            pltpu.make_async_remote_copy(
                src_ref=tot_out, dst_ref=tot_in.at[k], send_sem=tot_ssem.at[0], recv_sem=tot_rsem.at[k],
                device_id={"tm": jnp.int32(k), "space": sp}, device_id_type=MESH).wait_recv()
            state[...] = tot_in[k, 0:8] * state[...] + tot_in[k, 8:16]
    s = state[...]
    arrive = jnp.where(low8, s, roll_a * s + roll_b)[0:1]
    scaled = (keep[1] * arrive + keep[0]) * jnp.sqrt(2.0 * rr)
    scaled = jnp.concatenate([jnp.where(low, scaled, 0.0), jnp.where(low, 0.0, scaled)], axis=0).astype(BF16)

    def out_copy(k):
        return pltpu.make_async_copy(out_v.at[k], out.at[:, pl.ds(k * GB, GB), :], out_sem.at[k])

    for k in range(C // GB):
        for i in range(0, GB, 2):
            g = k * GB + i
            far = jnp.dot(scaled, jnp.concatenate([from_v[g], from_v[g + 1]], axis=1), preferred_element_type=F32)
            for u in range(2):
                live = (first + g + u).astype(F32) < act[...]
                pot = jnp.where(live, near[g + u] + far[:, u * E:(u + 1) * E], 0.0)
                stage[pl.ds(i + u, T, stride=GB), :] = pot
        out_v[k] = stage[...].reshape(T, GB, E).astype(BF16)
        out_copy(k).start()

    for k in range(C // GB):
        out_copy(k).wait()
    for d in range(1, n_space):
        part_copy(d).wait_send()
    for d in range(1, n_tm):
        @pl.when(tm + d < n_tm)
        def _(d=d):
            tot_copy(d).wait_send()
    for ds in (0, 1, -1):
        @pl.when(jnp.logical_and(has[1][0], on_space(ds)))
        def _(ds=ds):
            row_copy(ds).wait_send()
    for ds in (1, -1):
        @pl.when(on_space(ds))
        def _(ds=ds):
            halo_copy(ds).wait_send()


def solution(mesh):
    n_tm, n_space = mesh.shape["tm"], mesh.shape["space"]

    def local(density, active, neighbours, near_blocks, to_moments, from_moments, decay_rates, lengths):
        T, C, E = density.shape
        J = neighbours.shape[1]
        M = decay_rates.shape[0]
        H, W = T // 2, C + 2 * REACH
        vm = lambda shape, t: pltpu.VMEM(shape, t)
        dma = pltpu.SemaphoreType.DMA
        anyspec = pl.BlockSpec(memory_space=pl.ANY)
        vspec = pl.BlockSpec(memory_space=pltpu.VMEM)
        return pl.pallas_call(
            functools.partial(kernel, n_tm, n_space),
            out_shape=jax.ShapeDtypeStruct((T, C, E), BF16),
            in_specs=[anyspec, vspec, pl.BlockSpec(memory_space=pltpu.SMEM), anyspec, anyspec, anyspec, vspec, vspec],
            out_specs=anyspec,
            scratch_shapes=[
                vm((T, C, E), BF16), vm((T * C, E), F32), vm((W, T + PAD, E), BF16),
                vm((2, T, REACH, E), BF16), vm((8, 128), F32), vm((C, E), F32), vm((W, E), F32),
                vm((2, C, J, E, E), BF16), vm((M, C, E), BF16), vm((M, C, E), BF16),
                vm((C, 2 * M, E), BF16), vm((C, 2 * M, E), BF16),
                vm((C, T, E), F32), vm((T * 8, E), F32), vm((C // 8, T, 8, E), BF16), vm((T, 128), F32),
                vm((H, 2 * M), BF16), vm((n_space, H, 2 * M), BF16), vm((2, H, 2 * M), F32),
                vm((16, 2 * M), F32), vm((n_tm, 16, 2 * M), F32), vm((8, 2 * M), F32),
                dma((3,)), dma((C,)), dma((2, 2)), dma((2, 3)), dma((n_space,)), dma((n_space,)),
                dma((n_tm,)), dma((n_tm,)), dma((C // 8,)),
            ],
            compiler_params=pltpu.CompilerParams(
                collective_id=0, has_side_effects=True, vmem_limit_bytes=60 * 1024 * 1024),
        )(density, active.reshape(2, H), neighbours.T, near_blocks, to_moments, from_moments,
          decay_rates.reshape(1, M), lengths.reshape(2, H))

    placed = (
        P("tm", "space", None), P("tm"), P("space", None), P(None, "space", None, None, None),
        P(None, "space", None), P(None, "space", None), P(), P("tm"),
    )
    return jax.shard_map(
        local, mesh=mesh, in_specs=placed, out_specs=P("tm", "space", None), check_vma=False)
```

```python
import functools
import math

import jax
import jax.numpy as jnp
from jax import lax
from jax.experimental import pallas as pl
from jax.experimental.pallas import tpu as pltpu
from jax.sharding import PartitionSpec as P

REACH = 8
PAD = 16
VMEM = 67043328
MESH = pl.DeviceIdType.MESH
F32, BF16 = jnp.float32, jnp.bfloat16


def spread(row):
    return jnp.broadcast_to(row, (128, row.shape[1])).T


def kernel(n_tm, n_space, dens, active, nbrs, blocks, to_m, from_m, rates, lengths,
           near, from_v, act, scaled_o, dens_v, flat, work, halo, halo_prev, row_out, row_in, wb, to_raw, from_raw, to_v,
           part_out, part_in, keep, tot_out, tot_in, state,
           in_sem, w_sem, halo_sem, row_sem, part_ssem, part_rsem, tot_ssem, tot_rsem):
    T, C, E = dens_v.shape
    M = to_raw.shape[0]
    J = wb.shape[2]
    H = T // 2
    tm, sp = lax.axis_index("tm"), lax.axis_index("space")
    first = sp * C

    c_dens = pltpu.make_async_copy(dens, dens_v, in_sem.at[0])
    c_to = pltpu.make_async_copy(to_m, to_raw, in_sem.at[1])
    c_from = pltpu.make_async_copy(from_m, from_raw, in_sem.at[2])
    c_dens.start()
    c_to.start()
    barrier = pltpu.get_barrier_semaphore()

    def greet(t, s):
        pl.semaphore_signal(barrier, inc=1, device_id={"tm": t, "space": s}, device_id_type=MESH)

    for d in range(1, n_space):
        greet(tm, lax.rem(sp + d, n_space))
    for d in range(1, n_tm):
        greet(lax.rem(tm + d, n_tm), sp)
    one, nil = jnp.int32(1), jnp.int32(0)
    has = {-1: (tm > 0, sp > 0), 1: (tm < n_tm - 1, sp < n_space - 1)}
    corners = nil
    for dt in (-1, 1):
        for ds in (-1, 1):
            there = jnp.logical_and(has[dt][0], has[ds][1])
            corners = corners + jnp.where(there, one, nil)

            @pl.when(there)
            def _(dt=dt, ds=ds):
                greet(tm + dt, sp + ds)

    def w_copy(c):
        return pltpu.make_async_copy(blocks.at[:, c], wb.at[:, c], w_sem.at[c])

    for h in range(2):
        act[h * H:(h + 1) * H, :] = spread(active[h:h + 1, :].astype(F32))

    c_dens.wait()
    c_from.start()
    for lo, hi in ((REACH, C - REACH), (0, REACH), (C - REACH, C)):
        @pl.loop(lo, hi)
        def _(c):
            w_copy(c).start()

    gid = lax.broadcasted_iota(jnp.int32, (C, E), 0).astype(F32) + first.astype(F32)
    row_out[...] = jnp.where(gid < act[T - 1:T, :], dens_v[T - 1].astype(F32), 0.0)
    pl.semaphore_wait(barrier, n_space - 1 + n_tm - 1 + corners)

    def row_copy(ds):
        if ds == 0:
            src, dst = row_out, row_in.at[pl.ds(REACH, C)]
        elif ds == 1:
            src, dst = row_out.at[pl.ds(C - REACH, REACH)], row_in.at[pl.ds(0, REACH)]
        else:
            src, dst = row_out.at[pl.ds(0, REACH)], row_in.at[pl.ds(REACH + C, REACH)]
        return pltpu.make_async_remote_copy(
            src_ref=src, dst_ref=dst, send_sem=row_sem.at[0, ds + 1], recv_sem=row_sem.at[1, ds + 1],
            device_id={"tm": tm + 1, "space": sp + ds}, device_id_type=MESH)

    def halo_copy(ds):
        k = (1 - ds) // 2
        src = dens_v.at[:, pl.ds(C - REACH if ds == 1 else 0, REACH), :]
        return pltpu.make_async_remote_copy(
            src_ref=src, dst_ref=halo.at[k], send_sem=halo_sem.at[0, k], recv_sem=halo_sem.at[1, k],
            device_id={"tm": tm, "space": sp + ds}, device_id_type=MESH)

    def on_space(ds):
        return True if ds == 0 else has[ds][1]

    for ds in (0, 1, -1):
        @pl.when(jnp.logical_and(has[1][0], on_space(ds)))
        def _(ds=ds):
            row_copy(ds).start()
    for ds in (1, -1):
        @pl.when(on_space(ds))
        def _(ds=ds):
            halo_copy(ds).start()

    TB = 16

    def group(raw, n):
        @pl.loop(0, n // TB)
        def _(i):
            x = raw[pl.ds(i * TB, TB)].astype(F32)
            for q in range(C // 8):
                at = pl.multiple_of(q * n * 8 + i * TB * 8, TB * 8)
                flat[pl.ds(at, TB * 8), :] = x[:, q * 8:q * 8 + 8].reshape(TB * 8, E)

    def cluster(g, n):
        return flat[pl.ds(g // 8 * (n * 8) + g % 8, n, stride=8), :]

    group(dens_v, T)

    @pl.loop(0, C)
    def _(g):
        live = (first + g).astype(F32) < act[...]
        work[REACH + g, 0:T, :] = jnp.where(live, cluster(g, T), 0.0).astype(BF16)

    def expand(raw, dst):
        group(raw, M)

        @pl.loop(0, C)
        def _(g):
            x = cluster(g, M).astype(BF16)
            dst[g, 0:M, :] = x
            dst[g, M:2 * M, :] = x

    c_to.wait()
    expand(to_raw, to_v)

    lane = lax.broadcasted_iota(jnp.int32, (H, 2 * M), 1)
    low = lane < M
    total = jnp.zeros((T, 2 * M), F32)
    GB = 8
    for k in range(C // GB):
        a = jnp.concatenate([work[REACH + k * GB + i, 0:T, :] for i in range(GB)], axis=1)
        b = jnp.concatenate([to_v[k * GB + i] for i in range(GB)], axis=1)
        total = total + lax.dot_general(a, b, (((1,), (1,)), ((), ())), preferred_element_type=F32)
    part = jnp.where(low, total[0:H], total[H:T])
    keep[0] = part
    part_out[...] = part.astype(BF16)

    def part_copy(d):
        return pltpu.make_async_remote_copy(
            src_ref=part_out, dst_ref=part_in.at[sp], send_sem=part_ssem.at[d], recv_sem=part_rsem.at[sp],
            device_id={"tm": tm, "space": lax.rem(sp + d, n_space)}, device_id_type=MESH)

    for d in range(1, n_space):
        part_copy(d).start()

    c_from.wait()
    expand(from_raw, from_v)

    @pl.when(tm == 0)
    def _():
        row_in[...] = jnp.zeros_like(row_in)

    for ds in (0, 1, -1):
        there = has[-1][0] if ds == 0 else jnp.logical_and(has[-1][0], has[-ds][1])

        @pl.when(there)
        def _(ds=ds):
            row_copy(ds).wait_recv()
    top = lax.broadcasted_iota(jnp.int32, (PAD, E), 0) == 0

    @pl.loop(0, C + 2 * REACH)
    def _(g):
        r = jnp.broadcast_to(row_in[pl.ds(g, 1), :], (PAD, E))
        work[g, T:T + PAD, :] = jnp.where(top, r, 0.0).astype(BF16)

    first_row = lax.broadcasted_iota(jnp.int32, (T, E), 0) == 0

    def near_field(c):
        w_copy(c).wait()
        rows = [jnp.clip(nbrs[j, c] - first + REACH, 0, C + 2 * REACH - 1) for j in range(J)]
        picked = jnp.concatenate([work[i] for i in rows], axis=1)
        w = jnp.concatenate([wb[0, c].reshape(J * E, E), wb[1, c].reshape(J * E, E)], axis=1)
        both = jnp.dot(picked, w, preferred_element_type=F32)
        late = both[:, E:]
        late = jnp.where(first_row, late[T:T + 1, :], pltpu.roll(late[0:T], 1, 0))
        near[c] = both[0:T, 0:E] + late

    pl.loop(REACH, C - REACH)(near_field)

    moment = keep[0]
    for d in range(1, n_space):
        k = lax.rem(sp + n_space - d, n_space)
        pltpu.make_async_remote_copy(
            src_ref=part_out, dst_ref=part_in.at[k], send_sem=part_ssem.at[d], recv_sem=part_rsem.at[k],
            device_id={"tm": tm, "space": k}, device_id_type=MESH).wait_recv()
        moment = moment + part_in[k].astype(F32)
    r = rates[...]
    rr = jnp.concatenate([r, r], axis=1)
    span = jnp.where(low, spread(lengths[0:1, :]), spread(lengths[1:2, :]))
    fall = jnp.exp(-rr * span)
    pos = lax.broadcasted_iota(jnp.int32, (H, 2 * M), 0)
    d = 1
    while d < H:
        start = pos < d
        moment = fall * jnp.where(start, 0.0, pltpu.roll(moment, d, 0)) + moment
        fall = fall * jnp.where(start, 1.0, pltpu.roll(fall, d, 0))
        d *= 2
    keep[0] = jnp.where(pos < 1, 0.0, pltpu.roll(moment, 1, 0))
    keep[1] = jnp.where(pos < 1, 1.0, pltpu.roll(fall, 1, 0))
    end_b = jnp.broadcast_to(moment[H - 1:H, :], (8, 2 * M))
    end_a = jnp.broadcast_to(fall[H - 1:H, :], (8, 2 * M))
    low8 = low[0:8]
    roll_b, roll_a = pltpu.roll(end_b, M, 1), pltpu.roll(end_a, M, 1)
    tot_out[0:8] = end_a * roll_a
    tot_out[8:16] = jnp.where(low8, roll_a * end_b + roll_b, end_a * roll_b + end_b)

    def tot_copy(d):
        return pltpu.make_async_remote_copy(
            src_ref=tot_out, dst_ref=tot_in.at[tm], send_sem=tot_ssem.at[d], recv_sem=tot_rsem.at[tm],
            device_id={"tm": tm + d, "space": sp}, device_id_type=MESH)

    for d in range(1, n_tm):
        @pl.when(tm + d < n_tm)
        def _(d=d):
            tot_copy(d).start()

    for ds in (1, -1):
        k = (1 - ds) // 2

        @pl.when(on_space(-ds))
        def _(ds=ds, k=k):
            halo_copy(ds).wait_recv()

            @pl.loop(0, T // 32)
            def _(i):
                x = halo[k, pl.ds(i * 32, 32)].astype(F32)
                flat[pl.ds(pl.multiple_of(i * 32 * REACH, 32 * REACH), 32 * REACH), :] = x.reshape(32 * REACH, E)

            begin = 0 if k == 0 else REACH + C

            @pl.loop(0, REACH)
            def _(g):
                x = flat[pl.ds(g, T, stride=REACH), :]
                live = (first - REACH + begin + g).astype(F32) < act[...]
                work[begin + g, 0:T, :] = jnp.where(live, x, 0.0).astype(BF16)

    @pl.loop(0, 2 * REACH)
    def _(i):
        near_field(jnp.where(i < REACH, i, i + C - 2 * REACH))

    state[...] = jnp.zeros_like(state)
    for k in range(n_tm - 1):
        @pl.when(k < tm)
        def _(k=k):
            pltpu.make_async_remote_copy(
                src_ref=tot_out, dst_ref=tot_in.at[k], send_sem=tot_ssem.at[0], recv_sem=tot_rsem.at[k],
                device_id={"tm": jnp.int32(k), "space": sp}, device_id_type=MESH).wait_recv()
            state[...] = tot_in[k, 0:8] * state[...] + tot_in[k, 8:16]
    s = state[...]
    arrive = jnp.where(low8, s, roll_a * s + roll_b)[0:1]
    scaled = (keep[1] * arrive + keep[0]) * jnp.sqrt(2.0 * rr)
    scaled_o[0:H] = jnp.where(low, scaled, 0.0).astype(BF16)
    scaled_o[H:T] = jnp.where(low, 0.0, scaled).astype(BF16)


    for d in range(1, n_space):
        part_copy(d).wait_send()
    for d in range(1, n_tm):
        @pl.when(tm + d < n_tm)
        def _(d=d):
            tot_copy(d).wait_send()
    for ds in (0, 1, -1):
        @pl.when(jnp.logical_and(has[1][0], on_space(ds)))
        def _(ds=ds):
            row_copy(ds).wait_send()
    for ds in (1, -1):
        @pl.when(on_space(ds))
        def _(ds=ds):
            halo_copy(ds).wait_send()


def finish(near, from_v, act, scaled_o, out, stage, out_v, out_sem):
    C, T, E = near.shape
    GB = 8
    first = lax.axis_index("space") * C
    scaled = scaled_o[...]

    def out_copy(k):
        return pltpu.make_async_copy(out_v.at[k], out.at[:, pl.ds(k * GB, GB), :], out_sem.at[k])

    for k in range(C // GB):
        for i in range(0, GB, 2):
            g = k * GB + i
            far = jnp.dot(scaled, jnp.concatenate([from_v[g], from_v[g + 1]], axis=1), preferred_element_type=F32)
            for u in range(2):
                live = (first + g + u).astype(F32) < act[...]
                pot = jnp.where(live, near[g + u] + far[:, u * E:(u + 1) * E], 0.0)
                stage[pl.ds(i + u, T, stride=GB), :] = pot
        out_v[k] = stage[...].reshape(T, GB, E).astype(BF16)
        out_copy(k).start()
    for k in range(C // GB):
        out_copy(k).wait()


def solution(mesh):
    n_tm, n_space = mesh.shape["tm"], mesh.shape["space"]

    def local(density, active, neighbours, near_blocks, to_moments, from_moments, decay_rates, lengths):
        T, C, E = density.shape
        J = neighbours.shape[1]
        M = decay_rates.shape[0]
        H, W = T // 2, C + 2 * REACH
        vm = lambda shape, t: pltpu.VMEM(shape, t)
        dma = pltpu.SemaphoreType.DMA
        kept = [((C, T, E), F32), ((C, 2 * M, E), BF16), ((T, 128), F32), ((T, 2 * M), BF16)]
        room = sum(math.prod(s) * jnp.dtype(t).itemsize for s, t in kept) + 32 * 1024
        anyspec = pl.BlockSpec(memory_space=pl.ANY)
        vspec = pl.BlockSpec(memory_space=pltpu.VMEM)
        held = pl.pallas_call(
            functools.partial(kernel, n_tm, n_space),
            out_shape=[pltpu.VMEM(s, t) for s, t in kept],
            in_specs=[anyspec, vspec, pl.BlockSpec(memory_space=pltpu.SMEM), anyspec, anyspec, anyspec, vspec, vspec],
            out_specs=[vspec] * 4,
            scratch_shapes=[
                vm((T, C, E), BF16), vm((T * C, E), F32), vm((W, T + PAD, E), BF16),
                vm((2, T, REACH, E), BF16), vm((8, 128), F32), vm((C, E), F32), vm((W, E), F32),
                vm((2, C, J, E, E), BF16), vm((M, C, E), BF16), vm((M, C, E), BF16),
                vm((C, 2 * M, E), BF16),
                vm((H, 2 * M), BF16), vm((n_space, H, 2 * M), BF16), vm((2, H, 2 * M), F32),
                vm((16, 2 * M), F32), vm((n_tm, 16, 2 * M), F32), vm((8, 2 * M), F32),
                dma((3,)), dma((C,)), dma((2, 2)), dma((2, 3)), dma((n_space,)), dma((n_space,)),
                dma((n_tm,)), dma((n_tm,)),
            ],
            compiler_params=pltpu.CompilerParams(
                collective_id=0, has_side_effects=True, vmem_limit_bytes=VMEM - room),
        )(density, active.reshape(2, H), neighbours.T, near_blocks, to_moments, from_moments,
          decay_rates.reshape(1, M), lengths.reshape(2, H))
        return pl.pallas_call(
            finish,
            out_shape=jax.ShapeDtypeStruct((T, C, E), BF16),
            in_specs=[vspec] * 4,
            out_specs=anyspec,
            scratch_shapes=[vm((T * 8, E), F32), vm((C // 8, T, 8, E), BF16), dma((C // 8,))],
            compiler_params=pltpu.CompilerParams(vmem_limit_bytes=16 * 1024 * 1024),
        )(*held)

    placed = (
        P("tm", "space", None), P("tm"), P("space", None), P(None, "space", None, None, None),
        P(None, "space", None), P(None, "space", None), P(), P("tm"),
    )
    return jax.shard_map(
        local, mesh=mesh, in_specs=placed, out_specs=P("tm", "space", None), check_vma=False)
```

```python
import functools
import math

import jax
import jax.numpy as jnp
from jax import lax
from jax.experimental import pallas as pl
from jax.experimental.pallas import tpu as pltpu
from jax.sharding import PartitionSpec as P

REACH = 8
PAD = 16
VMEM = 67043328
MESH = pl.DeviceIdType.MESH
F32, BF16 = jnp.float32, jnp.bfloat16


def spread(row):
    return jnp.broadcast_to(row, (128, row.shape[1])).T


def kernel(n_tm, n_space, dens, active, nbrs, blocks, to_m, from_m, rates, lengths,
           near, from_v, act, scaled_o, dens_v, flat, work, halo, halo_prev, row_out, row_in, wb, to_raw, from_raw, to_v,
           part_out, part_in, keep, tot_out, tot_in, state,
           in_sem, w_sem, halo_sem, row_sem, part_ssem, part_rsem, tot_ssem, tot_rsem):
    T, C, E = dens_v.shape
    M = to_raw.shape[0]
    J = wb.shape[2]
    H = T // 2
    tm, sp = lax.axis_index("tm"), lax.axis_index("space")
    first = sp * C

    c_dens = pltpu.make_async_copy(dens, dens_v, in_sem.at[0])
    c_to = pltpu.make_async_copy(to_m, to_raw, in_sem.at[1])
    c_from = pltpu.make_async_copy(from_m, from_raw, in_sem.at[2])
    c_to.start()
    c_dens.start()
    c_from.start()
    barrier = pltpu.get_barrier_semaphore()

    def greet(t, s):
        pl.semaphore_signal(barrier, inc=1, device_id={"tm": t, "space": s}, device_id_type=MESH)

    for d in range(1, n_space):
        greet(tm, lax.rem(sp + d, n_space))
    for d in range(1, n_tm):
        greet(lax.rem(tm + d, n_tm), sp)
    one, nil = jnp.int32(1), jnp.int32(0)
    has = {-1: (tm > 0, sp > 0), 1: (tm < n_tm - 1, sp < n_space - 1)}
    corners = nil
    for dt in (-1, 1):
        for ds in (-1, 1):
            there = jnp.logical_and(has[dt][0], has[ds][1])
            corners = corners + jnp.where(there, one, nil)

            @pl.when(there)
            def _(dt=dt, ds=ds):
                greet(tm + dt, sp + ds)

    def w_copy(c):
        return pltpu.make_async_copy(blocks.at[:, c], wb.at[:, c], w_sem.at[c])

    for h in range(2):
        act[h * H:(h + 1) * H, :] = spread(active[h:h + 1, :].astype(F32))

    TB = 16

    def group(raw, n):
        @pl.loop(0, n // TB)
        def _(i):
            x = raw[pl.ds(i * TB, TB)].astype(F32)
            for q in range(C // 8):
                at = pl.multiple_of(q * n * 8 + i * TB * 8, TB * 8)
                flat[pl.ds(at, TB * 8), :] = x[:, q * 8:q * 8 + 8].reshape(TB * 8, E)

    def cluster(g, n):
        return flat[pl.ds(g // 8 * (n * 8) + g % 8, n, stride=8), :]

    def expand(raw, dst):
        group(raw, M)

        @pl.loop(0, C)
        def _(g):
            x = cluster(g, M).astype(BF16)
            dst[g, 0:M, :] = x
            dst[g, M:2 * M, :] = x

    c_to.wait()
    expand(to_raw, to_v)
    c_dens.wait()
    for lo, hi in ((REACH, C - REACH), (0, REACH), (C - REACH, C)):
        @pl.loop(lo, hi)
        def _(c):
            w_copy(c).start()

    gid = lax.broadcasted_iota(jnp.int32, (C, E), 0).astype(F32) + first.astype(F32)
    row_out[...] = jnp.where(gid < act[T - 1:T, :], dens_v[T - 1].astype(F32), 0.0)
    c_from.wait()
    expand(from_raw, from_v)
    pl.semaphore_wait(barrier, n_space - 1 + n_tm - 1 + corners)

    def row_copy(ds):
        if ds == 0:
            src, dst = row_out, row_in.at[pl.ds(REACH, C)]
        elif ds == 1:
            src, dst = row_out.at[pl.ds(C - REACH, REACH)], row_in.at[pl.ds(0, REACH)]
        else:
            src, dst = row_out.at[pl.ds(0, REACH)], row_in.at[pl.ds(REACH + C, REACH)]
        return pltpu.make_async_remote_copy(
            src_ref=src, dst_ref=dst, send_sem=row_sem.at[0, ds + 1], recv_sem=row_sem.at[1, ds + 1],
            device_id={"tm": tm + 1, "space": sp + ds}, device_id_type=MESH)

    def halo_copy(ds, h):
        k = (1 - ds) // 2
        return pltpu.make_async_remote_copy(
            src_ref=dens_v.at[pl.ds(h * H, H), pl.ds(C - REACH if ds == 1 else 0, REACH), :],
            dst_ref=halo.at[k, pl.ds(h * H, H)],
            send_sem=halo_sem.at[0, k, h], recv_sem=halo_sem.at[1, k, h],
            device_id={"tm": tm, "space": sp + ds}, device_id_type=MESH)

    def halo_send(h):
        for ds in (1, -1):
            @pl.when(on_space(ds))
            def _(ds=ds):
                halo_copy(ds, h).start()

    def on_space(ds):
        return True if ds == 0 else has[ds][1]

    for ds in (0, 1, -1):
        @pl.when(jnp.logical_and(has[1][0], on_space(ds)))
        def _(ds=ds):
            row_copy(ds).start()
    halo_send(0)

    group(dens_v, T)

    @pl.loop(0, C)
    def _(g):
        live = (first + g).astype(F32) < act[...]
        work[REACH + g, 0:T, :] = jnp.where(live, cluster(g, T), 0.0).astype(BF16)

    lane = lax.broadcasted_iota(jnp.int32, (H, 2 * M), 1)
    low = lane < M
    total = jnp.zeros((T, 2 * M), F32)
    GB = 8
    for k in range(C // GB):
        a = jnp.concatenate([work[REACH + k * GB + i, 0:T, :] for i in range(GB)], axis=1)
        b = jnp.concatenate([to_v[k * GB + i] for i in range(GB)], axis=1)
        total = total + lax.dot_general(a, b, (((1,), (1,)), ((), ())), preferred_element_type=F32)
    part = jnp.where(low, total[0:H], total[H:T])
    keep[0] = part
    part_out[...] = part.astype(BF16)

    def part_copy(d):
        return pltpu.make_async_remote_copy(
            src_ref=part_out, dst_ref=part_in.at[sp], send_sem=part_ssem.at[d], recv_sem=part_rsem.at[sp],
            device_id={"tm": tm, "space": lax.rem(sp + d, n_space)}, device_id_type=MESH)

    for d in range(1, n_space):
        part_copy(d).start()
    halo_send(1)

    @pl.when(tm == 0)
    def _():
        row_in[...] = jnp.zeros_like(row_in)

    for ds in (0, 1, -1):
        there = has[-1][0] if ds == 0 else jnp.logical_and(has[-1][0], has[-ds][1])

        @pl.when(there)
        def _(ds=ds):
            row_copy(ds).wait_recv()
    top = lax.broadcasted_iota(jnp.int32, (PAD, E), 0) == 0

    @pl.loop(0, C + 2 * REACH)
    def _(g):
        r = jnp.broadcast_to(row_in[pl.ds(g, 1), :], (PAD, E))
        work[g, T:T + PAD, :] = jnp.where(top, r, 0.0).astype(BF16)

    first_row = lax.broadcasted_iota(jnp.int32, (T, E), 0) == 0

    def near_field(c):
        w_copy(c).wait()
        rows = [jnp.clip(nbrs[j, c] - first + REACH, 0, C + 2 * REACH - 1) for j in range(J)]
        picked = jnp.concatenate([work[i] for i in rows], axis=1)
        w = jnp.concatenate([wb[0, c].reshape(J * E, E), wb[1, c].reshape(J * E, E)], axis=1)
        both = jnp.dot(picked, w, preferred_element_type=F32)
        late = both[:, E:]
        late = jnp.where(first_row, late[T:T + 1, :], pltpu.roll(late[0:T], 1, 0))
        near[c] = both[0:T, 0:E] + late

    pl.loop(REACH, C - REACH)(near_field)

    moment = keep[0]
    for d in range(1, n_space):
        k = lax.rem(sp + n_space - d, n_space)
        pltpu.make_async_remote_copy(
            src_ref=part_out, dst_ref=part_in.at[k], send_sem=part_ssem.at[d], recv_sem=part_rsem.at[k],
            device_id={"tm": tm, "space": k}, device_id_type=MESH).wait_recv()
        moment = moment + part_in[k].astype(F32)
    r = rates[...]
    rr = jnp.concatenate([r, r], axis=1)
    span = jnp.where(low, spread(lengths[0:1, :]), spread(lengths[1:2, :]))
    fall = jnp.exp(-rr * span)
    pos = lax.broadcasted_iota(jnp.int32, (H, 2 * M), 0)
    d = 1
    while d < H:
        start = pos < d
        moment = fall * jnp.where(start, 0.0, pltpu.roll(moment, d, 0)) + moment
        fall = fall * jnp.where(start, 1.0, pltpu.roll(fall, d, 0))
        d *= 2
    keep[0] = jnp.where(pos < 1, 0.0, pltpu.roll(moment, 1, 0))
    keep[1] = jnp.where(pos < 1, 1.0, pltpu.roll(fall, 1, 0))
    end_b = jnp.broadcast_to(moment[H - 1:H, :], (8, 2 * M))
    end_a = jnp.broadcast_to(fall[H - 1:H, :], (8, 2 * M))
    low8 = low[0:8]
    roll_b, roll_a = pltpu.roll(end_b, M, 1), pltpu.roll(end_a, M, 1)
    tot_out[0:8] = end_a * roll_a
    tot_out[8:16] = jnp.where(low8, roll_a * end_b + roll_b, end_a * roll_b + end_b)

    def tot_copy(d):
        return pltpu.make_async_remote_copy(
            src_ref=tot_out, dst_ref=tot_in.at[tm], send_sem=tot_ssem.at[d], recv_sem=tot_rsem.at[tm],
            device_id={"tm": tm + d, "space": sp}, device_id_type=MESH)

    for d in range(1, n_tm):
        @pl.when(tm + d < n_tm)
        def _(d=d):
            tot_copy(d).start()

    near_side = jnp.where(lax.rem(sp, 2) == 1, nil, one)
    for k in (near_side, one - near_side):
        other = sp + 2 * k - 1

        @pl.when(jnp.logical_and(other >= 0, other < n_space))
        def _(k=k, other=other):
            for h in range(2):
                pltpu.make_async_remote_copy(
                    src_ref=dens_v.at[pl.ds(h * H, H), pl.ds(0, REACH), :], dst_ref=halo.at[k, pl.ds(h * H, H)],
                    send_sem=halo_sem.at[0, k, h], recv_sem=halo_sem.at[1, k, h],
                    device_id={"tm": tm, "space": other}, device_id_type=MESH).wait_recv()

            @pl.loop(0, T // 32)
            def _(i):
                x = halo[k, pl.ds(i * 32, 32)].astype(F32)
                flat[pl.ds(pl.multiple_of(i * 32 * REACH, 32 * REACH), 32 * REACH), :] = x.reshape(32 * REACH, E)

            begin = k * (REACH + C)

            @pl.loop(0, REACH)
            def _(g):
                x = flat[pl.ds(g, T, stride=REACH), :]
                live = (first - REACH + begin + g).astype(F32) < act[...]
                work[begin + g, 0:T, :] = jnp.where(live, x, 0.0).astype(BF16)

        @pl.loop(0, REACH)
        def _(i):
            near_field(i + k * (C - REACH))

    state[...] = jnp.zeros_like(state)
    for k in range(n_tm - 1):
        @pl.when(k < tm)
        def _(k=k):
            pltpu.make_async_remote_copy(
                src_ref=tot_out, dst_ref=tot_in.at[k], send_sem=tot_ssem.at[0], recv_sem=tot_rsem.at[k],
                device_id={"tm": jnp.int32(k), "space": sp}, device_id_type=MESH).wait_recv()
            state[...] = tot_in[k, 0:8] * state[...] + tot_in[k, 8:16]
    s = state[...]
    arrive = jnp.where(low8, s, roll_a * s + roll_b)[0:1]
    scaled = (keep[1] * arrive + keep[0]) * jnp.sqrt(2.0 * rr)
    scaled_o[0:H] = jnp.where(low, scaled, 0.0).astype(BF16)
    scaled_o[H:T] = jnp.where(low, 0.0, scaled).astype(BF16)


    for d in range(1, n_space):
        part_copy(d).wait_send()
    for d in range(1, n_tm):
        @pl.when(tm + d < n_tm)
        def _(d=d):
            tot_copy(d).wait_send()
    for ds in (0, 1, -1):
        @pl.when(jnp.logical_and(has[1][0], on_space(ds)))
        def _(ds=ds):
            row_copy(ds).wait_send()
    for ds in (1, -1):
        @pl.when(on_space(ds))
        def _(ds=ds):
            for h in range(2):
                halo_copy(ds, h).wait_send()


def finish(near, from_v, act, scaled_o, out, stage, out_v, out_sem):
    C, T, E = near.shape
    GB = 8
    first = lax.axis_index("space") * C
    scaled = scaled_o[...]

    def out_copy(k):
        return pltpu.make_async_copy(out_v.at[k], out.at[:, pl.ds(k * GB, GB), :], out_sem.at[k])

    for k in range(C // GB):
        for i in range(0, GB, 2):
            g = k * GB + i
            far = jnp.dot(scaled, jnp.concatenate([from_v[g], from_v[g + 1]], axis=1), preferred_element_type=F32)
            for u in range(2):
                live = (first + g + u).astype(F32) < act[...]
                pot = jnp.where(live, near[g + u] + far[:, u * E:(u + 1) * E], 0.0)
                stage[pl.ds(i + u, T, stride=GB), :] = pot
        out_v[k] = stage[...].reshape(T, GB, E).astype(BF16)
        out_copy(k).start()
    for k in range(C // GB):
        out_copy(k).wait()


def solution(mesh):
    n_tm, n_space = mesh.shape["tm"], mesh.shape["space"]

    def local(density, active, neighbours, near_blocks, to_moments, from_moments, decay_rates, lengths):
        T, C, E = density.shape
        J = neighbours.shape[1]
        M = decay_rates.shape[0]
        H, W = T // 2, C + 2 * REACH
        vm = lambda shape, t: pltpu.VMEM(shape, t)
        dma = pltpu.SemaphoreType.DMA
        kept = [((C, T, E), F32), ((C, 2 * M, E), BF16), ((T, 128), F32), ((T, 2 * M), BF16)]
        room = sum(math.prod(s) * jnp.dtype(t).itemsize for s, t in kept) + 32 * 1024
        anyspec = pl.BlockSpec(memory_space=pl.ANY)
        vspec = pl.BlockSpec(memory_space=pltpu.VMEM)
        held = pl.pallas_call(
            functools.partial(kernel, n_tm, n_space),
            out_shape=[pltpu.VMEM(s, t) for s, t in kept],
            in_specs=[anyspec, vspec, pl.BlockSpec(memory_space=pltpu.SMEM), anyspec, anyspec, anyspec, vspec, vspec],
            out_specs=[vspec] * 4,
            scratch_shapes=[
                vm((T, C, E), BF16), vm((T * C, E), F32), vm((W, T + PAD, E), BF16),
                vm((2, T, REACH, E), BF16), vm((8, 128), F32), vm((C, E), F32), vm((W, E), F32),
                vm((2, C, J, E, E), BF16), vm((M, C, E), BF16), vm((M, C, E), BF16),
                vm((C, 2 * M, E), BF16),
                vm((H, 2 * M), BF16), vm((n_space, H, 2 * M), BF16), vm((2, H, 2 * M), F32),
                vm((16, 2 * M), F32), vm((n_tm, 16, 2 * M), F32), vm((8, 2 * M), F32),
                dma((3,)), dma((C,)), dma((2, 2, 2)), dma((2, 3)), dma((n_space,)), dma((n_space,)),
                dma((n_tm,)), dma((n_tm,)),
            ],
            compiler_params=pltpu.CompilerParams(
                collective_id=0, has_side_effects=True, vmem_limit_bytes=VMEM - room),
        )(density, active.reshape(2, H), neighbours.T, near_blocks, to_moments, from_moments,
          decay_rates.reshape(1, M), lengths.reshape(2, H))
        return pl.pallas_call(
            finish,
            out_shape=jax.ShapeDtypeStruct((T, C, E), BF16),
            in_specs=[vspec] * 4,
            out_specs=anyspec,
            scratch_shapes=[vm((T * 8, E), F32), vm((C // 8, T, 8, E), BF16), dma((C // 8,))],
            compiler_params=pltpu.CompilerParams(vmem_limit_bytes=16 * 1024 * 1024),
        )(*held)

    placed = (
        P("tm", "space", None), P("tm"), P("space", None), P(None, "space", None, None, None),
        P(None, "space", None), P(None, "space", None), P(), P("tm"),
    )
    return jax.shard_map(
        local, mesh=mesh, in_specs=placed, out_specs=P("tm", "space", None), check_vma=False)
```
